32 devices in a mesh: sta: 8 (over z, y), yr: 4 (over x, core).
Axes of the slice: x: 2, y: 2, z: 4, core: 2. Of those that a mesh axis runs over, the one named last changes fastest.
Arguments:
- temps: float32 [196608, 128], P(('sta', 'yr')), may hold values from -6 to 6
- day_bits: int32 [4, 196608], P(None, ('sta', 'yr')), may hold values from -2147483648 to 2147483646, as said below
- block_offset: int32 [196608], P(('sta', 'yr')), may hold values from 0 to 47
- block_counts: int32 [4, 2048], P('yr', 'sta'), may hold values from 0 to 48, as said below
- station_cell: int32 [2048], P('sta'), may hold values from 0 to 10367, as said below
Outputs:
- anomalies: float32 [196608, 128], P(('sta', 'yr'))
- climatology: float32 [10368, 384], P('sta')
The draws below stay inside these ranges and needn't reach their ends.
Inputs may be any that keep to these rules, and one draw needn't show every extreme that they name: `day_bits`: bit i of word w of a block's column says whether day 32 * w + i of the block was observed. `block_counts`: for each year range and station shard, the counts of the shard's 256 stations sum to 6144; in each of them some station has 48. `station_cell`: the owner of cell c is c // 1296. Of the 256 stations of one shard at most 128 lie in cells of one owner, and one owner has exactly 128 stations of every shard.
All inputs are finite; a program needn't handle non-finite values.
Results may differ from the reference program's by a relative error of at most 0.0003.
Values sent between devices are 32-bit elements; how exact they have to be, the bound alone decides.
A program may use at most 128 MiB of HBM per device.

```python
import jax
import jax.numpy as jnp
from jax import lax

DAYS = 128
CELLS = 10368
YR_DEV = 16
S_DEV = 256
MOST_BLOCKS = 48
BLK_DEV = 6144
STA_CAP = 128
STATIONS = 2048
BLOCKS = 196608


def draw_day_bits(key, part):
    return jax.random.randint(key, (DAYS // 32, BLOCKS), -2147483648, 2147483647, dtype=jnp.int32)


def draw_block_counts(key, part):
    shards = STATIONS // S_DEV
    groups = BLOCKS // BLK_DEV
    ranges = groups // shards
    half_most = MOST_BLOCKS // 2

    def group_counts(group_key):
        key_order, key_shift = jax.random.split(group_key)
        order_of = jax.random.permutation(key_order, S_DEV)
        shift_by = jax.random.randint(key_shift, (S_DEV // 2,), -half_most, half_most + 1, dtype=jnp.int32)
        shift_by = jnp.where(jnp.arange(S_DEV // 2, dtype=jnp.int32) == 0, half_most, shift_by)
        paired = jnp.concatenate([half_most + shift_by, half_most - shift_by]).astype(jnp.int32)
        return jnp.zeros((S_DEV,), jnp.int32).at[order_of].set(paired)
    counts = jax.vmap(group_counts)(jax.random.split(key, groups))
    return counts.reshape(ranges, shards * S_DEV).astype(jnp.int32)


def draw_station_cell(key, part):
    shards = STATIONS // S_DEV
    capacity = STA_CAP
    cell_dev = CELLS // shards
    key_hot, key_rest = jax.random.split(key)
    hot_owner = jax.random.randint(key_hot, (), 0, shards, dtype=jnp.int32)

    def shard_cells(shard_key):
        key_order, key_others, key_cell = jax.random.split(shard_key, 3)
        order_of = jax.random.permutation(key_order, S_DEV)
        others = (hot_owner + 1 + jax.random.permutation(key_others, shards - 1).astype(jnp.int32)) % shards
        slot_rank = jnp.arange(S_DEV, dtype=jnp.int32)
        group_of = jnp.clip((slot_rank - capacity) // (capacity // 2), 0, shards - 2)
        owner_ranked = jnp.where(slot_rank < capacity, hot_owner, others[group_of]).astype(jnp.int32)
        owner_of = jnp.zeros((S_DEV,), jnp.int32).at[order_of].set(owner_ranked)
        local_cell = jax.random.randint(key_cell, (S_DEV,), 0, cell_dev, dtype=jnp.int32)
        return owner_of * cell_dev + local_cell
    cells = jax.vmap(shard_cells)(jax.random.split(key_rest, shards))
    return cells.reshape(-1).astype(jnp.int32)


def set_ends(array, stream_key, least, top_value):
    place = [jax.random.randint(jax.random.fold_in(stream_key, axis), (), 0, length) for axis, length in enumerate(array.shape)]
    main_axis = array.shape.index(max(array.shape))
    next_to = place[:main_axis] + [(place[main_axis] + 1) % array.shape[main_axis]] + place[main_axis + 1:]
    return array.at[tuple(place)].set(least).at[tuple(next_to)].set(top_value)


def shard_levels(key, dims, cuts, least, high):
    level, own = 1.0, jax.random.fold_in(key, 6)
    for dim, shards_of in cuts:
        steps = jnp.exp(jax.random.uniform(jax.random.fold_in(own, dim), (shards_of,), jnp.float32, least / len(cuts), high / len(cuts)))
        level = level * jnp.repeat(steps, dims[dim] // shards_of).reshape([-1 if axis == dim else 1 for axis in range(len(dims))])
    return level


def gaussian(own_key, shape, spread, bound, cuts=(), kind=jnp.bfloat16):
    array = jax.random.normal(own_key, shape, jnp.float32) * spread
    if len(cuts) > 0:
        array = shard_levels(own_key, shape, cuts, -0.22, 0.18) * array
    return jnp.clip(array, min=-bound, max=bound).astype(kind)


def setup_inputs(seed: int = 0) -> dict:
    key_of = jax.random.split(jax.random.key(seed), 6)
    return {
        "temps": gaussian(key_of[0], (BLOCKS, DAYS), 1.0, 6.0, ((0, 32),), jnp.float32),
        "day_bits": draw_day_bits(jax.random.fold_in(key_of[5], 71), 0),
        "block_offset": set_ends(jax.random.randint(key_of[2], (BLOCKS,), 0, 3 * YR_DEV), jax.random.fold_in(key_of[2], 1), 0, (3 * YR_DEV) - 1).astype(jnp.int32),
        "block_counts": draw_block_counts(jax.random.fold_in(key_of[5], 71), 0),
        "station_cell": draw_station_cell(jax.random.fold_in(key_of[5], 71), 0),
    }


CALENDAR = 365


def observed_days(packed, offsets):
    day_count = packed.shape[0] * 32
    shifts = jnp.arange(32, dtype=jnp.int32)
    bit_values = jnp.right_shift(packed[:, None, :], shifts[None, :, None]) & 1
    bit_values = bit_values.reshape(day_count, packed.shape[1]).T
    thirds = (offsets % 3).astype(jnp.int32)
    season_day = thirds[:, None] * day_count + jnp.arange(day_count, dtype=jnp.int32)[None, :]
    observed = jnp.where((bit_values == 1) & (season_day < CALENDAR), 1.0, 0.0).astype(jnp.float32)
    return observed, thirds


def slot_stations(counts, block_total):
    ends_at = jnp.cumsum(counts).astype(jnp.int32)
    slot_ids = jnp.arange(block_total, dtype=jnp.int32)
    return jnp.searchsorted(ends_at, slot_ids, side="right").astype(jnp.int32)


def reference(temps, day_bits, block_offset, block_counts, station_cell):
    shards = STATIONS // S_DEV
    ranges = block_counts.shape[0]
    groups = shards * ranges
    row_width = 3 * DAYS
    temps_grouped = temps.reshape(groups, BLK_DEV, DAYS)
    packed_grouped = jnp.transpose(day_bits.reshape(DAYS // 32, groups, BLK_DEV), (1, 0, 2))
    offsets_grouped = block_offset.reshape(groups, BLK_DEV)
    counts_grouped = jnp.transpose(block_counts.reshape(ranges, shards, S_DEV), (1, 0, 2)).reshape(groups, S_DEV)

    def first_pass(inputs):
        values, packed, offsets, counts = inputs
        observed, thirds = observed_days(packed, offsets)
        segment = slot_stations(counts, BLK_DEV) * 3 + thirds
        total_sums = jax.ops.segment_sum(observed * values, segment, num_segments=S_DEV * 3)
        tallies = jax.ops.segment_sum(observed, segment, num_segments=S_DEV * 3)
        return total_sums.reshape(S_DEV, row_width), tallies.reshape(S_DEV, row_width)

    station_sums, station_tallies = lax.map(first_pass, (temps_grouped, packed_grouped, offsets_grouped, counts_grouped))
    station_sums = jnp.sum(station_sums.reshape(shards, ranges, S_DEV, row_width), axis=1).reshape(STATIONS, row_width)
    station_tallies = jnp.sum(station_tallies.reshape(shards, ranges, S_DEV, row_width), axis=1).reshape(STATIONS, row_width)
    cell_sums = jax.ops.segment_sum(station_sums, station_cell, num_segments=CELLS)
    cell_tallies = jax.ops.segment_sum(station_tallies, station_cell, num_segments=CELLS)
    climatology = cell_sums / jnp.maximum(cell_tallies, 1.0)
    station_clim = climatology[station_cell].reshape(shards, S_DEV * 3, DAYS)

    def second_pass(inputs):
        group_index, values, packed, offsets, counts = inputs
        observed, thirds = observed_days(packed, offsets)
        segment = slot_stations(counts, BLK_DEV) * 3 + thirds
        shard_clim = lax.dynamic_index_in_dim(station_clim, group_index // ranges, 0, keepdims=False)
        block_clim = shard_clim[segment]
        return observed * (values - block_clim)

    anomalies = lax.map(second_pass, (jnp.arange(groups, dtype=jnp.int32), temps_grouped, packed_grouped, offsets_grouped, counts_grouped))
    return anomalies.reshape(BLOCKS, DAYS), climatology
```

```python
import functools

import jax
import jax.numpy as jnp
from jax import lax
from jax.experimental import pallas as pl
from jax.experimental.pallas import tpu as pltpu
from jax.sharding import PartitionSpec as P

CELLS = 10368
CALENDAR = 365
MOST_BLOCKS = 48
LANES = 128
F32 = jnp.float32
BF16 = jnp.bfloat16


def round_up(value, step):
    return (value + step - 1) // step * step


def day_code(bits, offsets):
    rows = bits.shape[1]
    third = offsets - 3 * ((offsets * 21846) >> 16)
    words = jnp.concatenate(
        [jnp.broadcast_to(bits[w : w + 1], (32, rows)) for w in range(bits.shape[0])], axis=0
    )
    day = lax.broadcasted_iota(jnp.int32, words.shape, 0)
    bit = (words >> (day & 31)) & 1
    observed = jnp.where(third * LANES + day < CALENDAR, bit, 0)
    return third, (observed + 2 * third).astype(F32)


def split_two(value):
    high = value.astype(BF16)
    return high, (value - high.astype(F32)).astype(BF16)


def lane_group(rows, width):
    return lax.broadcasted_iota(jnp.int32, (rows, LANES), 1) // width


def gather_lanes(parts, shifts, width):
    group = lane_group(parts[0].shape[0], width)
    total = None
    for j, (part, shift) in enumerate(zip(parts, shifts)):
        shift = shift % LANES
        moved = pltpu.roll(part, shift, 1) if shift else part
        total = jnp.where(group == j, moved, 0.0 if total is None else total)
    return total


def sums_kernel(ranges, packed, temps_ref, bits_ref, offs_ref, counts_ref, out_ref, acc, edges):
    step = pl.program_id(0)
    rows = temps_ref.shape[0]
    stations = counts_ref.shape[1]

    @pl.when(step == 0)
    def _():
        acc[...] = jnp.zeros_like(acc)
        counts = jnp.broadcast_to(counts_ref[...].astype(F32), (stations, stations))
        at = lax.broadcasted_iota(jnp.int32, (stations, stations), 0)
        of = lax.broadcasted_iota(jnp.int32, (stations, stations), 1)
        ends = jnp.sum(jnp.where(of <= at, counts, 0.0), axis=1, keepdims=True)
        starts = jnp.sum(jnp.where(of < at, counts, 0.0), axis=1, keepdims=True)
        edges[0] = jnp.broadcast_to(starts, (stations, LANES)).astype(jnp.int32)
        edges[1] = jnp.broadcast_to(ends, (stations, LANES)).astype(jnp.int32)

    third, code = day_code(bits_ref[...], offs_ref[...])
    code = code.T
    observed = code - 2.0 * jnp.floor(code * 0.5)
    high, low = split_two(temps_ref[...] * observed)
    values = jnp.concatenate([high, low, observed.astype(BF16)], axis=1)
    row = lax.broadcasted_iota(jnp.int32, (1, rows), 1) + step * rows
    inside = (row >= edges[0][:, 0:1]) & (row < edges[1][:, 0:1])
    station_third = jnp.where(inside, third, 3)
    onehot = jnp.concatenate(
        [jnp.where(station_third == k, 1.0, 0.0).astype(BF16) for k in range(3)], axis=0
    )
    acc[...] += jnp.dot(onehot, values, preferred_element_type=F32)

    @pl.when(step == pl.num_programs(0) - 1)
    def _():
        width = LANES // ranges
        third_of = [acc[k * stations : (k + 1) * stations, :] for k in range(3)]
        groups = [t[:, :LANES] + t[:, LANES : 2 * LANES] for t in third_of]
        tallies = [t[:, 2 * LANES :] for t in third_of]
        if packed:
            groups.append(tallies[0] + 256.0 * tallies[1] + 65536.0 * tallies[2])
        else:
            groups.extend(tallies)
        for r in range(ranges):
            out_ref[r] = gather_lanes(groups, [width * (k - r) for k in range(len(groups))], width)


def cells_kernel(ranges, packed, cell_dev, cell_pad, got_ref, first_ref, own_ref, out_ref, acc):
    shards, _, _ = got_ref.shape
    stations = own_ref.shape[0]
    width = LANES // ranges
    ids = lax.broadcasted_iota(jnp.int32, (cell_pad, 1), 0).astype(F32) + first_ref[0, 0].astype(F32)
    acc[...] = jnp.zeros_like(acc)
    group = lane_group(stations, width)
    for s in range(shards):
        both = got_ref[s, :stations, :]
        high, low = split_two(both)
        if packed:
            tally = both.astype(jnp.int32)
            tally = jnp.where(
                group == 0,
                pltpu.roll(tally, LANES - 3 * width, 1) & 255,
                jnp.where(
                    group == 1,
                    (pltpu.roll(tally, LANES - 2 * width, 1) >> 8) & 255,
                    (pltpu.roll(tally, LANES - width, 1) >> 16) & 255,
                ),
            ).astype(F32)
            values = [high, low, tally.astype(BF16)]
        else:
            tally = pltpu.roll(both, LANES - 3 * width, 1)
            values = [high, low, *split_two(tally)]
        values = jnp.concatenate(values, axis=1)
        for q in range(stations // LANES):
            cells = got_ref[s, stations + q : stations + q + 1, :]
            part = values[q * LANES : (q + 1) * LANES]
            hot = jnp.where(ids == cells, 1.0, 0.0).astype(BF16)
            acc[:cell_pad] += jnp.dot(hot, part, preferred_element_type=F32)
            hot = jnp.where(own_ref[...] == cells, 1.0, 0.0).astype(BF16)
            acc[cell_pad:] += jnp.dot(hot, part, preferred_element_type=F32)
    tallies = acc[:, 2 * LANES : 3 * LANES]
    if not packed:
        tallies = tallies + acc[:, 3 * LANES :]
    acc[:, :LANES] = (acc[:, :LANES] + acc[:, LANES : 2 * LANES]) / jnp.maximum(tallies, 1.0)
    cell_rows, station_rows = cell_pad // ranges, stations // ranges
    for k in range(3):
        shifts = [width * (j - k) for j in range(ranges)]
        out_ref[k, :cell_rows] = gather_lanes(
            [acc[j * cell_rows : (j + 1) * cell_rows, :LANES] for j in range(ranges)], shifts, width
        )
        first = [cell_pad + j * station_rows for j in range(ranges)]
        out_ref[k, cell_rows:] = gather_lanes(
            [acc[f : f + station_rows, :LANES] for f in first], shifts, width
        )


def unpack(clim_ref, k, j, first, count, ranges, width):
    return gather_lanes(
        [clim_ref[r, k, first : first + count, :] for r in range(ranges)],
        [width * (r - j) for r in range(ranges)],
        width,
    )


def anomaly_kernel(
    ranges, cell_dev, cell_pad, temps_ref, bits_ref, offs_ref, counts_ref, clim_ref,
    out_ref, climatology_ref, edges, table,
):
    step = pl.program_id(0)
    rows = temps_ref.shape[0]
    stations = counts_ref.shape[1]
    width = LANES // ranges
    cell_rows, station_rows = cell_pad // ranges, stations // ranges

    @pl.when(step == 0)
    def _():
        at = lax.broadcasted_iota(jnp.int32, (stations, stations), 0)
        of = lax.broadcasted_iota(jnp.int32, (stations, stations), 1)
        counts = jnp.broadcast_to(counts_ref[...].astype(F32), (stations, stations))
        column = jnp.sum(jnp.where(at == of, counts, 0.0), axis=1, keepdims=True)
        ends = jnp.sum(jnp.where(at <= of, column, 0.0), axis=0, keepdims=True)
        edges[0:1] = (ends - counts_ref[...].astype(F32)).astype(jnp.int32)
        edges[1:2] = ends.astype(jnp.int32)
        for k in range(3):
            for j in range(ranges):
                part = unpack(clim_ref, k, j, cell_rows, station_rows, ranges, width)
                high, low = split_two(part)
                at_rows = slice(j * station_rows, (j + 1) * station_rows)
                table[at_rows, 2 * k * LANES : (2 * k + 1) * LANES] = high
                table[at_rows, (2 * k + 1) * LANES : (2 * k + 2) * LANES] = low
                count = min(cell_dev - j * cell_rows, cell_rows)
                if count > 0:
                    climatology_ref[
                        j * cell_rows : j * cell_rows + count, k * LANES : (k + 1) * LANES
                    ] = unpack(clim_ref, k, j, 0, count, ranges, width)

    _, code = day_code(bits_ref[...], offs_ref[...])
    code = code.T
    third = jnp.floor(code * 0.5)
    row = lax.broadcasted_iota(jnp.int32, (rows, stations), 0) + step * rows
    inside = (row >= edges[0:1]) & (row < edges[1:2])
    onehot = jnp.where(inside, 1.0, 0.0).astype(BF16)
    found = jnp.dot(onehot, table[...], preferred_element_type=F32)
    clim = [
        found[:, 2 * k * LANES : (2 * k + 1) * LANES]
        + found[:, (2 * k + 1) * LANES : (2 * k + 2) * LANES]
        for k in range(3)
    ]
    block_clim = jnp.where(third == 0.0, clim[0], jnp.where(third == 1.0, clim[1], clim[2]))
    out_ref[...] = (code - 2.0 * third) * (temps_ref[...] - block_clim)


def exchange_in(sums, cells, owners, ranges):
    mine = lax.psum_scatter(sums, "yr", scatter_dimension=0, tiled=False)
    return lax.all_gather(jnp.concatenate([mine, cells], axis=0), "sta")


def exchange_out(part, ranges):
    return lax.all_gather(part, "yr")


def per_device(temps, day_bits, block_offset, block_counts, station_cell):
    owners, ranges = lax.axis_size("sta"), lax.axis_size("yr")
    stations = station_cell.shape[0]
    block_total, day_count = temps.shape
    cell_dev = CELLS // owners
    cell_pad = round_up(cell_dev, 8 * ranges)
    packed = ranges * MOST_BLOCKS < 256
    rows = 1024 if block_total % 1024 == 0 else block_total
    offsets = block_offset.reshape(1, block_total)
    row_specs = [
        pl.BlockSpec((rows, day_count), lambda i: (i, 0)),
        pl.BlockSpec((day_bits.shape[0], rows), lambda i: (0, i)),
        pl.BlockSpec((1, rows), lambda i: (0, i)),
        pl.BlockSpec((1, stations), lambda i: (0, 0)),
    ]
    params = pltpu.CompilerParams(
        dimension_semantics=("arbitrary",), vmem_limit_bytes=48 * 1024 * 1024
    )
    sums = pl.pallas_call(
        functools.partial(sums_kernel, ranges, packed),
        grid=(block_total // rows,),
        in_specs=row_specs,
        out_specs=pl.BlockSpec((ranges, stations, LANES), lambda i: (0, 0, 0)),
        out_shape=jax.ShapeDtypeStruct((ranges, stations, LANES), F32),
        scratch_shapes=[
            pltpu.VMEM((3 * stations, 3 * LANES), F32),
            pltpu.VMEM((2, stations, LANES), jnp.int32),
        ],
        compiler_params=params,
    )(temps, day_bits, offsets, block_counts)

    cell_row_count = round_up(stations // LANES, 8)
    cell_rows = jnp.pad(
        station_cell.astype(F32).reshape(stations // LANES, LANES),
        ((0, cell_row_count - stations // LANES), (0, 0)),
    )
    got = exchange_in(sums, cell_rows, owners, ranges)

    first = (lax.axis_index("sta") * cell_dev).astype(jnp.int32).reshape(1, 1)
    part_rows = (cell_pad + stations) // ranges
    part = pl.pallas_call(
        functools.partial(cells_kernel, ranges, packed, cell_dev, cell_pad),
        in_specs=[
            pl.BlockSpec(memory_space=pltpu.VMEM),
            pl.BlockSpec(memory_space=pltpu.SMEM),
            pl.BlockSpec(memory_space=pltpu.VMEM),
        ],
        out_specs=pl.BlockSpec(memory_space=pltpu.VMEM),
        out_shape=jax.ShapeDtypeStruct((3, part_rows, LANES), F32),
        scratch_shapes=[pltpu.VMEM((cell_pad + stations, (3 if packed else 4) * LANES), F32)],
        compiler_params=pltpu.CompilerParams(vmem_limit_bytes=48 * 1024 * 1024),
    )(got, first, station_cell.astype(F32).reshape(stations, 1))

    parts = exchange_out(part, ranges)

    return pl.pallas_call(
        functools.partial(anomaly_kernel, ranges, cell_dev, cell_pad),
        grid=(block_total // rows,),
        in_specs=row_specs
        + [pl.BlockSpec((ranges, 3, part_rows, LANES), lambda i: (0, 0, 0, 0))],
        out_specs=[
            pl.BlockSpec((rows, day_count), lambda i: (i, 0)),
            pl.BlockSpec((cell_dev, 3 * LANES), lambda i: (0, 0)),
        ],
        out_shape=[
            jax.ShapeDtypeStruct((block_total, day_count), F32),
            jax.ShapeDtypeStruct((cell_dev, 3 * LANES), F32),
        ],
        scratch_shapes=[
            pltpu.VMEM((8, stations), jnp.int32),
            pltpu.VMEM((stations, 6 * LANES), BF16),
        ],
        compiler_params=params,
    )(temps, day_bits, offsets, block_counts, parts)


def solution(mesh):
    in_specs = (
        P(("sta", "yr"), None),
        P(None, ("sta", "yr")),
        P(("sta", "yr")),
        P("yr", "sta"),
        P("sta"),
    )
    out_specs = (P(("sta", "yr"), None), P("sta", None))

    def run(*args):
        return tuple(per_device(*args))

    return jax.shard_map(
        run, mesh=mesh, in_specs=in_specs, out_specs=out_specs, check_vma=False
    )
```

```python
import functools

import jax
import jax.numpy as jnp
from jax import lax
from jax.experimental import pallas as pl
from jax.experimental.pallas import tpu as pltpu
from jax.sharding import PartitionSpec as P

CELLS = 10368
CALENDAR = 365
MOST_BLOCKS = 48
LANES = 128
F32 = jnp.float32
BF16 = jnp.bfloat16


def round_up(value, step):
    return (value + step - 1) // step * step


def day_code(bits, offsets):
    rows = bits.shape[1]
    third = offsets - 3 * ((offsets * 21846) >> 16)
    words = jnp.concatenate(
        [jnp.broadcast_to(bits[w : w + 1], (32, rows)) for w in range(bits.shape[0])], axis=0
    )
    day = lax.broadcasted_iota(jnp.int32, words.shape, 0)
    bit = (words >> (day & 31)) & 1
    observed = jnp.where(third * LANES + day < CALENDAR, bit, 0)
    return third, (observed + 2 * third).astype(F32)


def split_two(value):
    high = value.astype(BF16)
    return high, (value - high.astype(F32)).astype(BF16)


def lane_group(rows, width):
    return lax.broadcasted_iota(jnp.int32, (rows, LANES), 1) // width


def gather_lanes(parts, shifts, width):
    group = lane_group(parts[0].shape[0], width)
    total = None
    for j, (part, shift) in enumerate(zip(parts, shifts)):
        shift = shift % LANES
        moved = pltpu.roll(part, shift, 1) if shift else part
        total = jnp.where(group == j, moved, 0.0 if total is None else total)
    return total


def sums_kernel(ranges, packed, temps_ref, bits_ref, offs_ref, counts_ref, out_ref, acc, edges):
    step = pl.program_id(0)
    rows = temps_ref.shape[0]
    stations = counts_ref.shape[1]

    @pl.when(step == 0)
    def _():
        acc[...] = jnp.zeros_like(acc)
        counts = jnp.broadcast_to(counts_ref[...].astype(F32), (stations, stations))
        at = lax.broadcasted_iota(jnp.int32, (stations, stations), 0)
        of = lax.broadcasted_iota(jnp.int32, (stations, stations), 1)
        ends = jnp.sum(jnp.where(of <= at, counts, 0.0), axis=1, keepdims=True)
        starts = jnp.sum(jnp.where(of < at, counts, 0.0), axis=1, keepdims=True)
        edges[0] = jnp.broadcast_to(starts, (stations, LANES)).astype(jnp.int32)
        edges[1] = jnp.broadcast_to(ends, (stations, LANES)).astype(jnp.int32)

    third, code = day_code(bits_ref[...], offs_ref[...])
    code = code.T
    observed = code - 2.0 * jnp.floor(code * 0.5)
    high, low = split_two(temps_ref[...] * observed)
    values = jnp.concatenate([high, low, observed.astype(BF16)], axis=1)
    row = lax.broadcasted_iota(jnp.int32, (1, rows), 1) + step * rows
    inside = (row >= edges[0][:, 0:1]) & (row < edges[1][:, 0:1])
    station_third = jnp.where(inside, third, 3)
    onehot = jnp.concatenate(
        [jnp.where(station_third == k, 1.0, 0.0).astype(BF16) for k in range(3)], axis=0
    )
    acc[...] += jnp.dot(onehot, values, preferred_element_type=F32)

    @pl.when(step == pl.num_programs(0) - 1)
    def _():
        width = LANES // ranges
        third_of = [acc[k * stations : (k + 1) * stations, :] for k in range(3)]
        groups = [t[:, :LANES] + t[:, LANES : 2 * LANES] for t in third_of]
        tallies = [t[:, 2 * LANES :] for t in third_of]
        if packed:
            groups.append(tallies[0] + 256.0 * tallies[1] + 65536.0 * tallies[2])
        else:
            groups.extend(tallies)
        for r in range(ranges):
            out_ref[r] = gather_lanes(groups, [width * (k - r) for k in range(len(groups))], width)


def cells_kernel(ranges, packed, cell_dev, cell_pad, got_ref, first_ref, own_ref, out_ref, acc):
    shards, _, _ = got_ref.shape
    stations = own_ref.shape[0]
    width = LANES // ranges
    ids = lax.broadcasted_iota(jnp.int32, (cell_pad, 1), 0).astype(F32) + first_ref[0, 0].astype(F32)
    acc[...] = jnp.zeros_like(acc)
    group = lane_group(stations, width)
    for s in range(shards):
        both = got_ref[s, :stations, :]
        high, low = split_two(both)
        if packed:
            tally = both.astype(jnp.int32)
            tally = jnp.where(
                group == 0,
                pltpu.roll(tally, LANES - 3 * width, 1) & 255,
                jnp.where(
                    group == 1,
                    (pltpu.roll(tally, LANES - 2 * width, 1) >> 8) & 255,
                    (pltpu.roll(tally, LANES - width, 1) >> 16) & 255,
                ),
            ).astype(F32)
            values = [high, low, tally.astype(BF16)]
        else:
            tally = pltpu.roll(both, LANES - 3 * width, 1)
            values = [high, low, *split_two(tally)]
        values = jnp.concatenate(values, axis=1)
        for q in range(stations // LANES):
            cells = got_ref[s, stations + q : stations + q + 1, :]
            part = values[q * LANES : (q + 1) * LANES]
            hot = jnp.where(ids == cells, 1.0, 0.0).astype(BF16)
            acc[:cell_pad] += jnp.dot(hot, part, preferred_element_type=F32)
            hot = jnp.where(own_ref[...] == cells, 1.0, 0.0).astype(BF16)
            acc[cell_pad:] += jnp.dot(hot, part, preferred_element_type=F32)
    tallies = acc[:, 2 * LANES : 3 * LANES]
    if not packed:
        tallies = tallies + acc[:, 3 * LANES :]
    acc[:, :LANES] = (acc[:, :LANES] + acc[:, LANES : 2 * LANES]) / jnp.maximum(tallies, 1.0)
    cell_rows, station_rows = cell_pad // ranges, stations // ranges
    for k in range(3):
        shifts = [width * (j - k) for j in range(ranges)]
        out_ref[k, :cell_rows] = gather_lanes(
            [acc[j * cell_rows : (j + 1) * cell_rows, :LANES] for j in range(ranges)], shifts, width
        )
        first = [cell_pad + j * station_rows for j in range(ranges)]
        out_ref[k, cell_rows:] = gather_lanes(
            [acc[f : f + station_rows, :LANES] for f in first], shifts, width
        )


def unpack(clim_ref, k, j, first, count, ranges, width):
    return gather_lanes(
        [clim_ref[r, k, first : first + count, :] for r in range(ranges)],
        [width * (r - j) for r in range(ranges)],
        width,
    )


def anomaly_kernel(
    ranges, cell_dev, cell_pad, temps_ref, bits_ref, offs_ref, counts_ref, clim_ref,
    out_ref, climatology_ref, edges, table,
):
    step = pl.program_id(0)
    rows = temps_ref.shape[0]
    stations = counts_ref.shape[1]
    width = LANES // ranges
    cell_rows, station_rows = cell_pad // ranges, stations // ranges

    @pl.when(step == 0)
    def _():
        at = lax.broadcasted_iota(jnp.int32, (stations, stations), 0)
        of = lax.broadcasted_iota(jnp.int32, (stations, stations), 1)
        counts = jnp.broadcast_to(counts_ref[...].astype(F32), (stations, stations))
        column = jnp.sum(jnp.where(at == of, counts, 0.0), axis=1, keepdims=True)
        ends = jnp.sum(jnp.where(at <= of, column, 0.0), axis=0, keepdims=True)
        edges[0:1] = (ends - counts_ref[...].astype(F32)).astype(jnp.int32)
        edges[1:2] = ends.astype(jnp.int32)
        for k in range(3):
            for j in range(ranges):
                part = unpack(clim_ref, k, j, cell_rows, station_rows, ranges, width)
                high, low = split_two(part)
                at_rows = slice(j * station_rows, (j + 1) * station_rows)
                table[at_rows, 2 * k * LANES : (2 * k + 1) * LANES] = high
                table[at_rows, (2 * k + 1) * LANES : (2 * k + 2) * LANES] = low
                count = min(cell_dev - j * cell_rows, cell_rows)
                if count > 0:
                    climatology_ref[
                        j * cell_rows : j * cell_rows + count, k * LANES : (k + 1) * LANES
                    ] = unpack(clim_ref, k, j, 0, count, ranges, width)

    _, code = day_code(bits_ref[...], offs_ref[...])
    code = code.T
    third = jnp.floor(code * 0.5)
    row = lax.broadcasted_iota(jnp.int32, (rows, stations), 0) + step * rows
    inside = (row >= edges[0:1]) & (row < edges[1:2])
    onehot = jnp.where(inside, 1.0, 0.0).astype(BF16)
    found = jnp.dot(onehot, table[...], preferred_element_type=F32)
    clim = [
        found[:, 2 * k * LANES : (2 * k + 1) * LANES]
        + found[:, (2 * k + 1) * LANES : (2 * k + 2) * LANES]
        for k in range(3)
    ]
    block_clim = jnp.where(third == 0.0, clim[0], jnp.where(third == 1.0, clim[1], clim[2]))
    out_ref[...] = (code - 2.0 * third) * (temps_ref[...] - block_clim)


def remote(src, dst, send, recv, where):
    return pltpu.make_async_remote_copy(
        src_ref=src, dst_ref=dst, send_sem=send, recv_sem=recv,
        device_id=where, device_id_type=pl.DeviceIdType.MESH,
    )


def greet(peers):
    barrier = pltpu.get_barrier_semaphore()
    for where in peers:
        pl.semaphore_signal(barrier, inc=1, device_id=where, device_id_type=pl.DeviceIdType.MESH)
    pl.semaphore_wait(barrier, len(peers))


def gather_kernel(
    owners, ranges, major, sums_ref, cells_ref, out_ref, pair, partial, across,
    pair_send, pair_recv, across_send, across_recv, far_send, far_recv, near_send, near_recv,
):
    stations = sums_ref.shape[1]
    chips, minor = ranges // 2, owners // major
    sta, yr = lax.axis_index("sta"), lax.axis_index("yr")
    chip, core = yr // 2, lax.rem(yr, 2)
    row, place = sta // minor, lax.rem(sta, minor)
    partner = {"yr": chip * 2 + 1 - core}
    chip_at = [lax.rem(chip + k, chips) for k in range(chips)]
    chip_from = [lax.rem(chip + chips - k, chips) for k in range(chips)]
    row_at = [lax.rem(row + k, major) for k in range(major)]
    row_from = [lax.rem(row + major - k, major) for k in range(major)]
    far = [{"sta": row_at[k] * minor + place} for k in range(1, major)]
    near = [{"sta": row * minor + lax.rem(place + j, minor)} for j in range(1, minor)]
    greet([partner] + [{"yr": c * 2 + core} for c in chip_at[1:]] + far + near)

    pairs = []
    for k in [*range(1, chips), 0]:
        copy = remote(
            sums_ref.at[chip_at[k] * 2 + 1 - core], pair.at[k],
            pair_send.at[k], pair_recv.at[k], partner,
        )
        copy.start()
        pairs.append(copy)
    crossing = []
    for k in range(1, chips):
        pairs[k - 1].wait_recv()
        partial[k - 1] = sums_ref[chip_at[k] * 2 + core] + pair[k]
        copy = remote(
            partial.at[k - 1], across.at[k - 1], across_send.at[k - 1], across_recv.at[k - 1],
            {"yr": chip_at[k] * 2 + core},
        )
        copy.start()
        crossing.append(copy)
    pairs[-1].wait_recv()
    total = sums_ref[yr] + pair[0]
    for k, copy in enumerate(crossing):
        copy.wait_recv()
        total = total + across[k]
    out_ref[sta, :stations] = total
    out_ref[sta, stations:] = cells_ref[...]

    sent = pairs + crossing
    fars, nears = [], []
    for k in range(1, major):
        copy = remote(
            out_ref.at[sta], out_ref.at[sta], far_send.at[k - 1], far_recv.at[k - 1], far[k - 1]
        )
        copy.start()
        fars.append(copy)
    for k in range(major):
        if k:
            fars[k - 1].wait_recv()
        block = row_from[k] * minor + place
        for j in range(1, minor):
            at = k * max(minor - 1, 1) + j - 1
            copy = remote(
                out_ref.at[block], out_ref.at[block], near_send.at[at], near_recv.at[at],
                near[j - 1],
            )
            copy.start()
            nears.append(copy)
    for copy in nears:
        copy.wait_recv()
    for copy in sent + fars + nears:
        copy.wait_send()


def exchange_in(sums, cells, owners, ranges):
    stations = sums.shape[1]
    major = 4 if owners % 4 == 0 else owners
    chips, minor = ranges // 2, owners // major
    block = stations + cells.shape[0]
    dma = pltpu.SemaphoreType.DMA
    near_count = max(major * (minor - 1), 1)
    crossings = max(chips - 1, 1)
    return pl.pallas_call(
        functools.partial(gather_kernel, owners, ranges, major),
        in_specs=[pl.BlockSpec(memory_space=pltpu.VMEM)] * 2,
        out_specs=pl.BlockSpec(memory_space=pltpu.VMEM),
        out_shape=jax.ShapeDtypeStruct((owners, block, LANES), F32),
        scratch_shapes=[
            pltpu.VMEM((chips, stations, LANES), F32),
            pltpu.VMEM((crossings, stations, LANES), F32),
            pltpu.VMEM((crossings, stations, LANES), F32),
            dma((chips,)), dma((chips,)), dma((crossings,)), dma((crossings,)),
            dma((max(major - 1, 1),)), dma((max(major - 1, 1),)), dma((near_count,)), dma((near_count,)),
        ],
        compiler_params=pltpu.CompilerParams(
            collective_id=0, has_side_effects=True, vmem_limit_bytes=48 * 1024 * 1024
        ),
    )(sums, cells)


def spread_kernel(ranges, part_ref, out_ref, far_send, far_recv, near_send, near_recv):
    chips = ranges // 2
    chunks = part_ref.shape[0]
    yr = lax.axis_index("yr")
    chip, core = yr // 2, lax.rem(yr, 2)
    partner = {"yr": chip * 2 + 1 - core}
    others = [lax.rem(chip + k, chips) * 2 + core for k in range(1, chips)]
    origins = [lax.rem(chip + chips - k, chips) * 2 + core for k in range(1, chips)]
    greet([partner] + [{"yr": other} for other in others])
    fars, nears = [], []
    for t in range(chunks):
        for k, other in enumerate(others):
            at = t * len(others) + k
            copy = remote(
                part_ref.at[t], out_ref.at[yr, t], far_send.at[at], far_recv.at[at], {"yr": other}
            )
            copy.start()
            fars.append(copy)
    for t in range(chunks):
        copy = remote(part_ref.at[t], out_ref.at[yr, t], near_send.at[t], near_recv.at[t], partner)
        copy.start()
        nears.append(copy)
    out_ref[yr] = part_ref[...]
    for t in range(chunks):
        for k, origin in enumerate(origins):
            at = t * len(others) + k
            fars[at].wait_recv()
            at = chunks + at
            copy = remote(
                out_ref.at[origin, t], out_ref.at[origin, t], near_send.at[at], near_recv.at[at],
                partner,
            )
            copy.start()
            nears.append(copy)
    for copy in nears:
        copy.wait_recv()
    for copy in fars + nears:
        copy.wait_send()


def exchange_out(part, ranges):
    chunks = part.shape[0]
    crossings = chunks * (ranges // 2 - 1)
    dma = pltpu.SemaphoreType.DMA
    return pl.pallas_call(
        functools.partial(spread_kernel, ranges),
        in_specs=[pl.BlockSpec(memory_space=pltpu.VMEM)],
        out_specs=pl.BlockSpec(memory_space=pltpu.VMEM),
        out_shape=jax.ShapeDtypeStruct((ranges, *part.shape), F32),
        scratch_shapes=[
            dma((max(crossings, 1),)), dma((max(crossings, 1),)),
            dma((chunks + crossings,)), dma((chunks + crossings,)),
        ],
        compiler_params=pltpu.CompilerParams(
            collective_id=1, has_side_effects=True, vmem_limit_bytes=48 * 1024 * 1024
        ),
    )(part)


def per_device(temps, day_bits, block_offset, block_counts, station_cell):
    owners, ranges = lax.axis_size("sta"), lax.axis_size("yr")
    stations = station_cell.shape[0]
    block_total, day_count = temps.shape
    cell_dev = CELLS // owners
    cell_pad = round_up(cell_dev, 8 * ranges)
    packed = ranges * MOST_BLOCKS < 256
    rows = 1024 if block_total % 1024 == 0 else block_total
    offsets = block_offset.reshape(1, block_total)
    row_specs = [
        pl.BlockSpec((rows, day_count), lambda i: (i, 0)),
        pl.BlockSpec((day_bits.shape[0], rows), lambda i: (0, i)),
        pl.BlockSpec((1, rows), lambda i: (0, i)),
        pl.BlockSpec((1, stations), lambda i: (0, 0)),
    ]
    params = pltpu.CompilerParams(
        dimension_semantics=("arbitrary",), vmem_limit_bytes=48 * 1024 * 1024
    )
    sums = pl.pallas_call(
        functools.partial(sums_kernel, ranges, packed),
        grid=(block_total // rows,),
        in_specs=row_specs,
        out_specs=pl.BlockSpec((ranges, stations, LANES), lambda i: (0, 0, 0)),
        out_shape=jax.ShapeDtypeStruct((ranges, stations, LANES), F32),
        scratch_shapes=[
            pltpu.VMEM((3 * stations, 3 * LANES), F32),
            pltpu.VMEM((2, stations, LANES), jnp.int32),
        ],
        compiler_params=params,
    )(temps, day_bits, offsets, block_counts)

    cell_row_count = round_up(stations // LANES, 8)
    cell_rows = jnp.pad(
        station_cell.astype(F32).reshape(stations // LANES, LANES),
        ((0, cell_row_count - stations // LANES), (0, 0)),
    )
    got = exchange_in(sums, cell_rows, owners, ranges)

    first = (lax.axis_index("sta") * cell_dev).astype(jnp.int32).reshape(1, 1)
    part_rows = (cell_pad + stations) // ranges
    part = pl.pallas_call(
        functools.partial(cells_kernel, ranges, packed, cell_dev, cell_pad),
        in_specs=[
            pl.BlockSpec(memory_space=pltpu.VMEM),
            pl.BlockSpec(memory_space=pltpu.SMEM),
            pl.BlockSpec(memory_space=pltpu.VMEM),
        ],
        out_specs=pl.BlockSpec(memory_space=pltpu.VMEM),
        out_shape=jax.ShapeDtypeStruct((3, part_rows, LANES), F32),
        scratch_shapes=[pltpu.VMEM((cell_pad + stations, (3 if packed else 4) * LANES), F32)],
        compiler_params=pltpu.CompilerParams(vmem_limit_bytes=48 * 1024 * 1024),
    )(got, first, station_cell.astype(F32).reshape(stations, 1))

    parts = exchange_out(part, ranges)

    return pl.pallas_call(
        functools.partial(anomaly_kernel, ranges, cell_dev, cell_pad),
        grid=(block_total // rows,),
        in_specs=row_specs
        + [pl.BlockSpec((ranges, 3, part_rows, LANES), lambda i: (0, 0, 0, 0))],
        out_specs=[
            pl.BlockSpec((rows, day_count), lambda i: (i, 0)),
            pl.BlockSpec((cell_dev, 3 * LANES), lambda i: (0, 0)),
        ],
        out_shape=[
            jax.ShapeDtypeStruct((block_total, day_count), F32),
            jax.ShapeDtypeStruct((cell_dev, 3 * LANES), F32),
        ],
        scratch_shapes=[
            pltpu.VMEM((8, stations), jnp.int32),
            pltpu.VMEM((stations, 6 * LANES), BF16),
        ],
        compiler_params=params,
    )(temps, day_bits, offsets, block_counts, parts)


def solution(mesh):
    in_specs = (
        P(("sta", "yr"), None),
        P(None, ("sta", "yr")),
        P(("sta", "yr")),
        P("yr", "sta"),
        P("sta"),
    )
    out_specs = (P(("sta", "yr"), None), P("sta", None))

    def run(*args):
        return tuple(per_device(*args))

    return jax.shard_map(
        run, mesh=mesh, in_specs=in_specs, out_specs=out_specs, check_vma=False
    )
```

```python
import functools

import jax
import jax.numpy as jnp
from jax import lax
from jax.experimental import pallas as pl
from jax.experimental.pallas import tpu as pltpu
from jax.sharding import PartitionSpec as P

CELLS = 10368
CALENDAR = 365
MOST_BLOCKS = 48
LANES = 128
F32 = jnp.float32
BF16 = jnp.bfloat16


def round_up(value, step):
    return (value + step - 1) // step * step


def day_code(bits, offsets):
    rows = bits.shape[1]
    third = offsets - 3 * ((offsets * 21846) >> 16)
    words = jnp.concatenate(
        [jnp.broadcast_to(bits[w : w + 1], (32, rows)) for w in range(bits.shape[0])], axis=0
    )
    day = lax.broadcasted_iota(jnp.int32, words.shape, 0)
    bit = (words >> (day & 31)) & 1
    observed = jnp.where(third * LANES + day < CALENDAR, bit, 0)
    return third, (observed + 2 * third).astype(F32)


def split_two(value):
    high = value.astype(BF16)
    return high, (value - high.astype(F32)).astype(BF16)


def lane_group(rows, width):
    return lax.broadcasted_iota(jnp.int32, (rows, LANES), 1) // width


def gather_lanes(parts, shifts, width):
    group = lane_group(parts[0].shape[0], width)
    total = None
    for j, (part, shift) in enumerate(zip(parts, shifts)):
        shift = shift % LANES
        moved = pltpu.roll(part, shift, 1) if shift else part
        total = jnp.where(group == j, moved, 0.0 if total is None else total)
    return total


def sums_kernel(ranges, packed, temps_ref, bits_ref, offs_ref, counts_ref, out_ref, acc, edges):
    step = pl.program_id(0)
    rows = temps_ref.shape[0]
    stations = counts_ref.shape[1]

    @pl.when(step == 0)
    def _():
        acc[...] = jnp.zeros_like(acc)
        counts = jnp.broadcast_to(counts_ref[...].astype(F32), (stations, stations))
        at = lax.broadcasted_iota(jnp.int32, (stations, stations), 0)
        of = lax.broadcasted_iota(jnp.int32, (stations, stations), 1)
        ends = jnp.sum(jnp.where(of <= at, counts, 0.0), axis=1, keepdims=True)
        starts = jnp.sum(jnp.where(of < at, counts, 0.0), axis=1, keepdims=True)
        edges[0] = jnp.broadcast_to(starts, (stations, LANES)).astype(jnp.int32)
        edges[1] = jnp.broadcast_to(ends, (stations, LANES)).astype(jnp.int32)

    third, code = day_code(bits_ref[...], offs_ref[...])
    code = code.T
    observed = code - 2.0 * jnp.floor(code * 0.5)
    high, low = split_two(temps_ref[...] * observed)
    values = jnp.concatenate([high, low, observed.astype(BF16)], axis=1)
    row = lax.broadcasted_iota(jnp.int32, (1, rows), 1) + step * rows
    inside = (row >= edges[0][:, 0:1]) & (row < edges[1][:, 0:1])
    station_third = jnp.where(inside, third, 3)
    onehot = jnp.concatenate(
        [jnp.where(station_third == k, 1.0, 0.0).astype(BF16) for k in range(3)], axis=0
    )
    acc[...] += jnp.dot(onehot, values, preferred_element_type=F32)

    @pl.when(step == pl.num_programs(0) - 1)
    def _():
        width = LANES // ranges
        third_of = [acc[k * stations : (k + 1) * stations, :] for k in range(3)]
        groups = [t[:, :LANES] + t[:, LANES : 2 * LANES] for t in third_of]
        tallies = [t[:, 2 * LANES :] for t in third_of]
        if packed:
            groups.append(tallies[0] + 256.0 * tallies[1] + 65536.0 * tallies[2])
        else:
            groups.extend(tallies)
        for r in range(ranges):
            out_ref[r] = gather_lanes(groups, [width * (k - r) for k in range(len(groups))], width)


def cells_kernel(ranges, packed, cell_dev, cell_pad, got_ref, first_ref, own_ref, out_ref, acc):
    shards, _, _ = got_ref.shape
    stations = own_ref.shape[0]
    width = LANES // ranges
    ids = lax.broadcasted_iota(jnp.int32, (cell_pad, 1), 0).astype(F32) + first_ref[0, 0].astype(F32)
    acc[...] = jnp.zeros_like(acc)
    group = lane_group(stations, width)
    for s in range(shards):
        both = got_ref[s, :stations, :]
        high, low = split_two(both)
        if packed:
            tally = both.astype(jnp.int32)
            tally = jnp.where(
                group == 0,
                pltpu.roll(tally, LANES - 3 * width, 1) & 255,
                jnp.where(
                    group == 1,
                    (pltpu.roll(tally, LANES - 2 * width, 1) >> 8) & 255,
                    (pltpu.roll(tally, LANES - width, 1) >> 16) & 255,
                ),
            ).astype(F32)
            values = [high, low, tally.astype(BF16)]
        else:
            tally = pltpu.roll(both, LANES - 3 * width, 1)
            values = [high, low, *split_two(tally)]
        values = jnp.concatenate(values, axis=1)
        for q in range(stations // LANES):
            cells = got_ref[s, stations + q : stations + q + 1, :]
            part = values[q * LANES : (q + 1) * LANES]
            hot = jnp.where(ids == cells, 1.0, 0.0).astype(BF16)
            acc[:cell_pad] += jnp.dot(hot, part, preferred_element_type=F32)
            hot = jnp.where(own_ref[...] == cells, 1.0, 0.0).astype(BF16)
            acc[cell_pad:] += jnp.dot(hot, part, preferred_element_type=F32)
    tallies = acc[:, 2 * LANES : 3 * LANES]
    if not packed:
        tallies = tallies + acc[:, 3 * LANES :]
    acc[:, :LANES] = (acc[:, :LANES] + acc[:, LANES : 2 * LANES]) / jnp.maximum(tallies, 1.0)
    cell_rows, station_rows = cell_pad // ranges, stations // ranges
    for k in range(3):
        shifts = [width * (j - k) for j in range(ranges)]
        out_ref[k, :cell_rows] = gather_lanes(
            [acc[j * cell_rows : (j + 1) * cell_rows, :LANES] for j in range(ranges)], shifts, width
        )
        first = [cell_pad + j * station_rows for j in range(ranges)]
        out_ref[k, cell_rows:] = gather_lanes(
            [acc[f : f + station_rows, :LANES] for f in first], shifts, width
        )


def unpack(clim_ref, k, j, first, count, ranges, width):
    return gather_lanes(
        [clim_ref[r, k, first : first + count, :] for r in range(ranges)],
        [width * (r - j) for r in range(ranges)],
        width,
    )


def anomaly_kernel(
    ranges, cell_dev, cell_pad, temps_ref, bits_ref, offs_ref, counts_ref, clim_ref,
    out_ref, climatology_ref, edges, table,
):
    step = pl.program_id(0)
    rows = temps_ref.shape[0]
    stations = counts_ref.shape[1]
    width = LANES // ranges
    cell_rows, station_rows = cell_pad // ranges, stations // ranges

    @pl.when(step == 0)
    def _():
        at = lax.broadcasted_iota(jnp.int32, (stations, stations), 0)
        of = lax.broadcasted_iota(jnp.int32, (stations, stations), 1)
        counts = jnp.broadcast_to(counts_ref[...].astype(F32), (stations, stations))
        column = jnp.sum(jnp.where(at == of, counts, 0.0), axis=1, keepdims=True)
        ends = jnp.sum(jnp.where(at <= of, column, 0.0), axis=0, keepdims=True)
        edges[0:1] = (ends - counts_ref[...].astype(F32)).astype(jnp.int32)
        edges[1:2] = ends.astype(jnp.int32)
        for k in range(3):
            for j in range(ranges):
                part = unpack(clim_ref, k, j, cell_rows, station_rows, ranges, width)
                high, low = split_two(part)
                at_rows = slice(j * station_rows, (j + 1) * station_rows)
                table[at_rows, 2 * k * LANES : (2 * k + 1) * LANES] = high
                table[at_rows, (2 * k + 1) * LANES : (2 * k + 2) * LANES] = low
                count = min(cell_dev - j * cell_rows, cell_rows)
                if count > 0:
                    climatology_ref[
                        j * cell_rows : j * cell_rows + count, k * LANES : (k + 1) * LANES
                    ] = unpack(clim_ref, k, j, 0, count, ranges, width)

    _, code = day_code(bits_ref[...], offs_ref[...])
    code = code.T
    third = jnp.floor(code * 0.5)
    row = lax.broadcasted_iota(jnp.int32, (rows, stations), 0) + step * rows
    inside = (row >= edges[0:1]) & (row < edges[1:2])
    onehot = jnp.where(inside, 1.0, 0.0).astype(BF16)
    found = jnp.dot(onehot, table[...], preferred_element_type=F32)
    clim = [
        found[:, 2 * k * LANES : (2 * k + 1) * LANES]
        + found[:, (2 * k + 1) * LANES : (2 * k + 2) * LANES]
        for k in range(3)
    ]
    block_clim = jnp.where(third == 0.0, clim[0], jnp.where(third == 1.0, clim[1], clim[2]))
    out_ref[...] = (code - 2.0 * third) * (temps_ref[...] - block_clim)


def remote(src, dst, send, recv, where):
    return pltpu.make_async_remote_copy(
        src_ref=src, dst_ref=dst, send_sem=send, recv_sem=recv,
        device_id=where, device_id_type=pl.DeviceIdType.MESH,
    )


def greet(peers, maybe=(), maybe_count=0):
    barrier = pltpu.get_barrier_semaphore()
    for where in peers:
        pl.semaphore_signal(barrier, inc=1, device_id=where, device_id_type=pl.DeviceIdType.MESH)
    for able, where in maybe:
        @pl.when(able)
        def _():
            pl.semaphore_signal(
                barrier, inc=1, device_id=where, device_id_type=pl.DeviceIdType.MESH
            )
    pl.semaphore_wait(barrier, len(peers) + maybe_count)


def gather_kernel(
    owners, ranges, major, sums_ref, cells_ref, out_ref, pair, partial, across,
    pair_send, pair_recv, across_send, across_recv, far_send, far_recv, near_send, near_recv,
):
    stations = sums_ref.shape[1]
    chips, minor = ranges // 2, owners // major
    sta, yr = lax.axis_index("sta"), lax.axis_index("yr")
    chip, core = yr // 2, lax.rem(yr, 2)
    row, place = sta // minor, lax.rem(sta, minor)
    partner = {"yr": chip * 2 + 1 - core}
    chip_at = [lax.rem(chip + k, chips) for k in range(chips)]
    chip_from = [lax.rem(chip + chips - k, chips) for k in range(chips)]
    near_peers = [{"sta": row * minor + lax.rem(place + j, minor)} for j in range(1, minor)]
    can_up, can_down = row < major - 1, row > 0

    def up(d):
        block = out_ref.at[(row - (d - 1)) * minor + place]
        return remote(
            block, block, far_send.at[0, d - 1], far_recv.at[0, d - 1],
            {"sta": (row + 1) * minor + place},
        )

    def down(d):
        block = out_ref.at[(row + (d - 1)) * minor + place]
        return remote(
            block, block, far_send.at[1, d - 1], far_recv.at[1, d - 1],
            {"sta": (row - 1) * minor + place},
        )

    def near(side, d):
        block = out_ref.at[(row + (d if side else -d)) * minor + place]
        return [
            remote(
                block, block, near_send.at[side, d, j], near_recv.at[side, d, j], near_peers[j]
            )
            for j in range(minor - 1)
        ]

    greet(
        [partner] + [{"yr": c * 2 + core} for c in chip_at[1:]] + near_peers,
        [
            (can_up, {"sta": (row + 1) * minor + place}),
            (can_down, {"sta": (row - 1) * minor + place}),
        ],
        (2 * (major - 1) - row) // major + (row + major - 1) // major,
    )

    pairs = []
    for k in [*range(1, chips), 0]:
        copy = remote(
            sums_ref.at[chip_at[k] * 2 + 1 - core], pair.at[k],
            pair_send.at[k], pair_recv.at[k], partner,
        )
        copy.start()
        pairs.append(copy)
    crossing = []
    for k in range(1, chips):
        pairs[k - 1].wait_recv()
        partial[k - 1] = sums_ref[chip_at[k] * 2 + core] + pair[k]
        copy = remote(
            partial.at[k - 1], across.at[k - 1], across_send.at[k - 1], across_recv.at[k - 1],
            {"yr": chip_at[k] * 2 + core},
        )
        copy.start()
        crossing.append(copy)
    pairs[-1].wait_recv()
    total = sums_ref[yr] + pair[0]
    for k, copy in enumerate(crossing):
        copy.wait_recv()
        total = total + across[k]
    out_ref[sta, :stations] = total
    out_ref[sta, stations:] = cells_ref[...]

    for able, copy_of in ((can_up, up), (can_down, down)):
        @pl.when(able)
        def _():
            copy_of(1).start()
    for copy in near(0, 0):
        copy.start()
    for d in range(1, major):
        for side, have, able, copy_of in (
            (0, row >= d, can_up, up), (1, row + d < major, can_down, down)
        ):
            @pl.when(have)
            def _():
                copy_of(d).wait_recv()
                if d + 1 < major:
                    @pl.when(able)
                    def _():
                        copy_of(d + 1).start()
                for copy in near(side, d):
                    copy.start()
    for copy in near(0, 0):
        copy.wait()
    for d in range(1, major):
        for side, have, able, copy_of in (
            (0, row >= d, can_up, up), (1, row + d < major, can_down, down)
        ):
            @pl.when(have)
            def _():
                for copy in near(side, d):
                    copy.wait()
            reach = (row >= d - 1) if side == 0 else (row + d - 1 < major)

            @pl.when(reach & able)
            def _():
                copy_of(d).wait_send()
    for copy in pairs + crossing:
        copy.wait_send()


def exchange_in(sums, cells, owners, ranges):
    stations = sums.shape[1]
    major = 4 if owners % 4 == 0 else owners
    chips, minor = ranges // 2, owners // major
    block = stations + cells.shape[0]
    dma = pltpu.SemaphoreType.DMA
    hops, near_count = max(major - 1, 1), max(minor - 1, 1)
    crossings = max(chips - 1, 1)
    return pl.pallas_call(
        functools.partial(gather_kernel, owners, ranges, major),
        in_specs=[pl.BlockSpec(memory_space=pltpu.VMEM)] * 2,
        out_specs=pl.BlockSpec(memory_space=pltpu.VMEM),
        out_shape=jax.ShapeDtypeStruct((owners, block, LANES), F32),
        scratch_shapes=[
            pltpu.VMEM((chips, stations, LANES), F32),
            pltpu.VMEM((crossings, stations, LANES), F32),
            pltpu.VMEM((crossings, stations, LANES), F32),
            dma((chips,)), dma((chips,)), dma((crossings,)), dma((crossings,)),
            dma((2, hops)), dma((2, hops)), dma((2, major, near_count)), dma((2, major, near_count)),
        ],
        compiler_params=pltpu.CompilerParams(
            collective_id=0, has_side_effects=True, vmem_limit_bytes=48 * 1024 * 1024
        ),
    )(sums, cells)


def spread_kernel(ranges, part_ref, out_ref, far_send, far_recv, near_send, near_recv):
    chips = ranges // 2
    chunks = part_ref.shape[0]
    yr = lax.axis_index("yr")
    chip, core = yr // 2, lax.rem(yr, 2)
    partner = {"yr": chip * 2 + 1 - core}
    others = [lax.rem(chip + k, chips) * 2 + core for k in range(1, chips)]
    origins = [lax.rem(chip + chips - k, chips) * 2 + core for k in range(1, chips)]
    greet([partner] + [{"yr": other} for other in others])
    fars, nears = [], []
    for t in range(chunks):
        for k, other in enumerate(others):
            at = t * len(others) + k
            copy = remote(
                part_ref.at[t], out_ref.at[yr, t], far_send.at[at], far_recv.at[at], {"yr": other}
            )
            copy.start()
            fars.append(copy)
    for t in range(chunks):
        copy = remote(part_ref.at[t], out_ref.at[yr, t], near_send.at[t], near_recv.at[t], partner)
        copy.start()
        nears.append(copy)
    out_ref[yr] = part_ref[...]
    for t in range(chunks):
        for k, origin in enumerate(origins):
            at = t * len(others) + k
            fars[at].wait_recv()
            at = chunks + at
            copy = remote(
                out_ref.at[origin, t], out_ref.at[origin, t], near_send.at[at], near_recv.at[at],
                partner,
            )
            copy.start()
            nears.append(copy)
    for copy in nears:
        copy.wait_recv()
    for copy in fars + nears:
        copy.wait_send()


def exchange_out(part, ranges):
    chunks = part.shape[0]
    crossings = chunks * (ranges // 2 - 1)
    dma = pltpu.SemaphoreType.DMA
    return pl.pallas_call(
        functools.partial(spread_kernel, ranges),
        in_specs=[pl.BlockSpec(memory_space=pltpu.VMEM)],
        out_specs=pl.BlockSpec(memory_space=pltpu.VMEM),
        out_shape=jax.ShapeDtypeStruct((ranges, *part.shape), F32),
        scratch_shapes=[
            dma((max(crossings, 1),)), dma((max(crossings, 1),)),
            dma((chunks + crossings,)), dma((chunks + crossings,)),
        ],
        compiler_params=pltpu.CompilerParams(
            collective_id=1, has_side_effects=True, vmem_limit_bytes=48 * 1024 * 1024
        ),
    )(part)


def per_device(temps, day_bits, block_offset, block_counts, station_cell):
    owners, ranges = lax.axis_size("sta"), lax.axis_size("yr")
    stations = station_cell.shape[0]
    block_total, day_count = temps.shape
    cell_dev = CELLS // owners
    cell_pad = round_up(cell_dev, 8 * ranges)
    packed = ranges * MOST_BLOCKS < 256
    rows = 1024 if block_total % 1024 == 0 else block_total
    offsets = block_offset.reshape(1, block_total)
    row_specs = [
        pl.BlockSpec((rows, day_count), lambda i: (i, 0)),
        pl.BlockSpec((day_bits.shape[0], rows), lambda i: (0, i)),
        pl.BlockSpec((1, rows), lambda i: (0, i)),
        pl.BlockSpec((1, stations), lambda i: (0, 0)),
    ]
    params = pltpu.CompilerParams(
        dimension_semantics=("arbitrary",), vmem_limit_bytes=48 * 1024 * 1024
    )
    wide = pltpu.CompilerParams(dimension_semantics=("arbitrary",), vmem_limit_bytes=67043328)
    sums = pl.pallas_call(
        functools.partial(sums_kernel, ranges, packed),
        grid=(block_total // rows,),
        in_specs=row_specs,
        out_specs=pl.BlockSpec((ranges, stations, LANES), lambda i: (0, 0, 0)),
        out_shape=jax.ShapeDtypeStruct((ranges, stations, LANES), F32),
        scratch_shapes=[
            pltpu.VMEM((3 * stations, 3 * LANES), F32),
            pltpu.VMEM((2, stations, LANES), jnp.int32),
        ],
        compiler_params=wide,
    )(temps, day_bits, offsets, block_counts)

    cell_row_count = round_up(stations // LANES, 8)
    cell_rows = jnp.pad(
        station_cell.astype(F32).reshape(stations // LANES, LANES),
        ((0, cell_row_count - stations // LANES), (0, 0)),
    )
    got = exchange_in(sums, cell_rows, owners, ranges)

    first = (lax.axis_index("sta") * cell_dev).astype(jnp.int32).reshape(1, 1)
    part_rows = (cell_pad + stations) // ranges
    part = pl.pallas_call(
        functools.partial(cells_kernel, ranges, packed, cell_dev, cell_pad),
        in_specs=[
            pl.BlockSpec(memory_space=pltpu.VMEM),
            pl.BlockSpec(memory_space=pltpu.SMEM),
            pl.BlockSpec(memory_space=pltpu.VMEM),
        ],
        out_specs=pl.BlockSpec(memory_space=pltpu.VMEM),
        out_shape=jax.ShapeDtypeStruct((3, part_rows, LANES), F32),
        scratch_shapes=[pltpu.VMEM((cell_pad + stations, (3 if packed else 4) * LANES), F32)],
        compiler_params=pltpu.CompilerParams(vmem_limit_bytes=48 * 1024 * 1024),
    )(got, first, station_cell.astype(F32).reshape(stations, 1))

    parts = exchange_out(part, ranges)

    return pl.pallas_call(
        functools.partial(anomaly_kernel, ranges, cell_dev, cell_pad),
        grid=(block_total // rows,),
        in_specs=row_specs
        + [pl.BlockSpec((ranges, 3, part_rows, LANES), lambda i: (0, 0, 0, 0))],
        out_specs=[
            pl.BlockSpec((rows, day_count), lambda i: (i, 0)),
            pl.BlockSpec((cell_dev, 3 * LANES), lambda i: (0, 0)),
        ],
        out_shape=[
            jax.ShapeDtypeStruct((block_total, day_count), F32),
            jax.ShapeDtypeStruct((cell_dev, 3 * LANES), F32),
        ],
        scratch_shapes=[
            pltpu.VMEM((8, stations), jnp.int32),
            pltpu.VMEM((stations, 6 * LANES), BF16),
        ],
        compiler_params=params,
    )(temps, day_bits, offsets, block_counts, parts)


def solution(mesh):
    in_specs = (
        P(("sta", "yr"), None),
        P(None, ("sta", "yr")),
        P(("sta", "yr")),
        P("yr", "sta"),
        P("sta"),
    )
    out_specs = (P(("sta", "yr"), None), P("sta", None))

    def run(*args):
        return tuple(per_device(*args))

    return jax.shard_map(
        run, mesh=mesh, in_specs=in_specs, out_specs=out_specs, check_vma=False
    )
```

```python
import functools

import jax
import jax.numpy as jnp
from jax import lax
from jax.experimental import pallas as pl
from jax.experimental.pallas import tpu as pltpu
from jax.sharding import PartitionSpec as P

CELLS = 10368
CALENDAR = 365
MOST_BLOCKS = 48
LANES = 128
F32 = jnp.float32
BF16 = jnp.bfloat16


def round_up(value, step):
    return (value + step - 1) // step * step


def day_code(bits, offsets):
    rows = bits.shape[1]
    third = offsets - 3 * ((offsets * 21846) >> 16)
    words = jnp.concatenate(
        [jnp.broadcast_to(bits[w : w + 1], (32, rows)) for w in range(bits.shape[0])], axis=0
    )
    day = lax.broadcasted_iota(jnp.int32, words.shape, 0)
    bit = (words >> (day & 31)) & 1
    observed = jnp.where(third * LANES + day < CALENDAR, bit, 0)
    return third, (observed + 2 * third).astype(F32)


def split_two(value):
    high = value.astype(BF16)
    return high, (value - high.astype(F32)).astype(BF16)


def lane_group(rows, width):
    return lax.broadcasted_iota(jnp.int32, (rows, LANES), 1) // width


def gather_lanes(parts, shifts, width):
    group = lane_group(parts[0].shape[0], width)
    total = None
    for j, (part, shift) in enumerate(zip(parts, shifts)):
        shift = shift % LANES
        moved = pltpu.roll(part, shift, 1) if shift else part
        total = jnp.where(group == j, moved, 0.0 if total is None else total)
    return total


def sums_kernel(ranges, packed, temps_ref, bits_ref, offs_ref, counts_ref, out_ref, acc, edges):
    step = pl.program_id(0)
    rows = temps_ref.shape[0]
    stations = counts_ref.shape[1]

    @pl.when(step == 0)
    def _():
        acc[...] = jnp.zeros_like(acc)
        counts = jnp.broadcast_to(counts_ref[...].astype(F32), (stations, stations))
        at = lax.broadcasted_iota(jnp.int32, (stations, stations), 0)
        of = lax.broadcasted_iota(jnp.int32, (stations, stations), 1)
        ends = jnp.sum(jnp.where(of <= at, counts, 0.0), axis=1, keepdims=True)
        starts = jnp.sum(jnp.where(of < at, counts, 0.0), axis=1, keepdims=True)
        edges[0] = jnp.broadcast_to(starts, (stations, LANES)).astype(jnp.int32)
        edges[1] = jnp.broadcast_to(ends, (stations, LANES)).astype(jnp.int32)

    third, code = day_code(bits_ref[...], offs_ref[...])
    code = code.T
    observed = code - 2.0 * jnp.floor(code * 0.5)
    high, low = split_two(temps_ref[...] * observed)
    values = jnp.concatenate([high, low, observed.astype(BF16)], axis=1)
    row = lax.broadcasted_iota(jnp.int32, (1, rows), 1) + step * rows
    inside = (row >= edges[0][:, 0:1]) & (row < edges[1][:, 0:1])
    station_third = jnp.where(inside, third, 3)
    onehot = jnp.concatenate(
        [jnp.where(station_third == k, 1.0, 0.0).astype(BF16) for k in range(3)], axis=0
    )
    acc[...] += jnp.dot(onehot, values, preferred_element_type=F32)

    @pl.when(step == pl.num_programs(0) - 1)
    def _():
        width = LANES // ranges
        third_of = [acc[k * stations : (k + 1) * stations, :] for k in range(3)]
        groups = [t[:, :LANES] + t[:, LANES : 2 * LANES] for t in third_of]
        tallies = [t[:, 2 * LANES :] for t in third_of]
        if packed:
            groups.append(tallies[0] + 256.0 * tallies[1] + 65536.0 * tallies[2])
        else:
            groups.extend(tallies)
        for r in range(ranges):
            out_ref[r] = gather_lanes(groups, [width * (k - r) for k in range(len(groups))], width)


def cell_chunks(ranges, cell_pad, stations):
    cell_rows, station_rows = cell_pad // ranges, stations // ranges
    step = round_up((cell_rows + 2) // 3, 8)
    edges = [*range(0, cell_rows, step), cell_rows]
    return [(cell_rows, cell_rows + station_rows)] + list(zip(edges[:-1], edges[1:]))


def cells_kernel(
    ranges, packed, cell_dev, cell_pad, got_ref, own_ref, out_ref, values, acc,
    far_send, far_recv, near_send, near_recv,
):
    shards, _, _ = got_ref.shape
    stations = own_ref.shape[0]
    width = LANES // ranges
    chips = ranges // 2
    yr = lax.axis_index("yr")
    chip, core = yr // 2, lax.rem(yr, 2)
    partner = {"yr": chip * 2 + 1 - core}
    others = [lax.rem(chip + k, chips) * 2 + core for k in range(1, chips)]
    origins = [lax.rem(chip + chips - k, chips) * 2 + core for k in range(1, chips)]
    greet([partner] + [{"yr": other} for other in others])
    group = lane_group(stations, width)
    for s in range(shards):
        both = got_ref[s, :stations, :]
        high, low = split_two(both)
        if packed:
            tally = both.astype(jnp.int32)
            tally = jnp.where(
                group == 0,
                pltpu.roll(tally, LANES - 3 * width, 1) & 255,
                jnp.where(
                    group == 1,
                    (pltpu.roll(tally, LANES - 2 * width, 1) >> 8) & 255,
                    (pltpu.roll(tally, LANES - width, 1) >> 16) & 255,
                ),
            ).astype(F32)
            columns = [high, low, tally.astype(BF16)]
        else:
            tally = pltpu.roll(both, LANES - 3 * width, 1)
            columns = [high, low, *split_two(tally)]
        values[s * stations : (s + 1) * stations] = jnp.concatenate(columns, axis=1)
    first = lax.axis_index("sta") * cell_dev
    cell_rows = cell_pad // ranges
    fars, nears = [], []
    for c, (low_row, high_row) in enumerate(cell_chunks(ranges, cell_pad, stations)):
        count = high_row - low_row
        if low_row == cell_rows:
            ids = own_ref[...]
        else:
            ids = jnp.concatenate(
                [
                    lax.broadcasted_iota(jnp.int32, (count, 1), 0) + (first + j * cell_rows + low_row)
                    for j in range(ranges)
                ],
                axis=0,
            ).astype(F32)
        total = ranges * count
        acc[:total] = jnp.zeros((total, acc.shape[1]), F32)
        for s in range(shards):
            hot = jnp.concatenate(
                [
                    jnp.where(ids == got_ref[s, q : q + 1, :], 1.0, 0.0).astype(BF16)
                    for q in range(stations, stations + stations // LANES)
                ],
                axis=1,
            )
            acc[:total] += jnp.dot(
                hot, values[s * stations : (s + 1) * stations], preferred_element_type=F32
            )
        tallies = acc[:total, 2 * LANES : 3 * LANES]
        if not packed:
            tallies = tallies + acc[:total, 3 * LANES :]
        clim = (acc[:total, :LANES] + acc[:total, LANES : 2 * LANES]) / jnp.maximum(tallies, 1.0)
        for k in range(3):
            out_ref[yr, k, low_row:high_row] = gather_lanes(
                [clim[j * count : (j + 1) * count] for j in range(ranges)],
                [width * (j - k) for j in range(ranges)],
                width,
            )
        block = out_ref.at[yr, :, low_row:high_row, :]
        for k, other in enumerate(others):
            copy = remote(block, block, far_send.at[c, k], far_recv.at[c, k], {"yr": other})
            copy.start()
            fars.append(copy)
        copy = remote(block, block, near_send.at[c, chips - 1], near_recv.at[c, chips - 1], partner)
        copy.start()
        nears.append(copy)
    for c, (low_row, high_row) in enumerate(cell_chunks(ranges, cell_pad, stations)):
        for k, origin in enumerate(origins):
            fars[c * len(origins) + k].wait_recv()
            block = out_ref.at[origin, :, low_row:high_row, :]
            copy = remote(block, block, near_send.at[c, k], near_recv.at[c, k], partner)
            copy.start()
            nears.append(copy)
    for copy in nears:
        copy.wait_recv()
    for copy in fars + nears:
        copy.wait_send()


def unpack(clim_ref, k, j, first, count, ranges, width):
    return gather_lanes(
        [clim_ref[r, k, first : first + count, :] for r in range(ranges)],
        [width * (r - j) for r in range(ranges)],
        width,
    )


def anomaly_kernel(
    ranges, cell_dev, cell_pad, temps_ref, bits_ref, offs_ref, counts_ref, clim_ref,
    out_ref, climatology_ref, edges, table,
):
    step = pl.program_id(0)
    rows = temps_ref.shape[0]
    stations = counts_ref.shape[1]
    width = LANES // ranges
    cell_rows, station_rows = cell_pad // ranges, stations // ranges

    @pl.when(step == 0)
    def _():
        at = lax.broadcasted_iota(jnp.int32, (stations, stations), 0)
        of = lax.broadcasted_iota(jnp.int32, (stations, stations), 1)
        counts = jnp.broadcast_to(counts_ref[...].astype(F32), (stations, stations))
        column = jnp.sum(jnp.where(at == of, counts, 0.0), axis=1, keepdims=True)
        ends = jnp.sum(jnp.where(at <= of, column, 0.0), axis=0, keepdims=True)
        edges[0:1] = (ends - counts_ref[...].astype(F32)).astype(jnp.int32)
        edges[1:2] = ends.astype(jnp.int32)
        for k in range(3):
            for j in range(ranges):
                part = unpack(clim_ref, k, j, cell_rows, station_rows, ranges, width)
                high, low = split_two(part)
                at_rows = slice(j * station_rows, (j + 1) * station_rows)
                table[at_rows, 2 * k * LANES : (2 * k + 1) * LANES] = high
                table[at_rows, (2 * k + 1) * LANES : (2 * k + 2) * LANES] = low
                count = min(cell_dev - j * cell_rows, cell_rows)
                if count > 0:
                    climatology_ref[
                        j * cell_rows : j * cell_rows + count, k * LANES : (k + 1) * LANES
                    ] = unpack(clim_ref, k, j, 0, count, ranges, width)

    _, code = day_code(bits_ref[...], offs_ref[...])
    code = code.T
    third = jnp.floor(code * 0.5)
    row = lax.broadcasted_iota(jnp.int32, (rows, stations), 0) + step * rows
    inside = (row >= edges[0:1]) & (row < edges[1:2])
    onehot = jnp.where(inside, 1.0, 0.0).astype(BF16)
    found = jnp.dot(onehot, table[...], preferred_element_type=F32)
    clim = [
        found[:, 2 * k * LANES : (2 * k + 1) * LANES]
        + found[:, (2 * k + 1) * LANES : (2 * k + 2) * LANES]
        for k in range(3)
    ]
    block_clim = jnp.where(third == 0.0, clim[0], jnp.where(third == 1.0, clim[1], clim[2]))
    out_ref[...] = (code - 2.0 * third) * (temps_ref[...] - block_clim)


def remote(src, dst, send, recv, where):
    return pltpu.make_async_remote_copy(
        src_ref=src, dst_ref=dst, send_sem=send, recv_sem=recv,
        device_id=where, device_id_type=pl.DeviceIdType.MESH,
    )


def greet(peers, maybe=(), maybe_count=0):
    barrier = pltpu.get_barrier_semaphore()
    for where in peers:
        pl.semaphore_signal(barrier, inc=1, device_id=where, device_id_type=pl.DeviceIdType.MESH)
    for able, where in maybe:
        @pl.when(able)
        def _():
            pl.semaphore_signal(
                barrier, inc=1, device_id=where, device_id_type=pl.DeviceIdType.MESH
            )
    pl.semaphore_wait(barrier, len(peers) + maybe_count)


def gather_kernel(
    owners, ranges, major, sums_ref, cells_ref, out_ref, pair, partial, across,
    pair_send, pair_recv, across_send, across_recv, far_send, far_recv, near_send, near_recv,
):
    stations = sums_ref.shape[1]
    chips, minor = ranges // 2, owners // major
    sta, yr = lax.axis_index("sta"), lax.axis_index("yr")
    chip, core = yr // 2, lax.rem(yr, 2)
    row, place = sta // minor, lax.rem(sta, minor)
    partner = {"yr": chip * 2 + 1 - core}
    chip_at = [lax.rem(chip + k, chips) for k in range(chips)]
    chip_from = [lax.rem(chip + chips - k, chips) for k in range(chips)]
    near_peers = [{"sta": row * minor + lax.rem(place + j, minor)} for j in range(1, minor)]
    can_up, can_down = row < major - 1, row > 0

    def up(d):
        block = out_ref.at[(row - (d - 1)) * minor + place]
        return remote(
            block, block, far_send.at[0, d - 1], far_recv.at[0, d - 1],
            {"sta": (row + 1) * minor + place},
        )

    def down(d):
        block = out_ref.at[(row + (d - 1)) * minor + place]
        return remote(
            block, block, far_send.at[1, d - 1], far_recv.at[1, d - 1],
            {"sta": (row - 1) * minor + place},
        )

    def near(side, d):
        block = out_ref.at[(row + (d if side else -d)) * minor + place]
        return [
            remote(
                block, block, near_send.at[side, d, j], near_recv.at[side, d, j], near_peers[j]
            )
            for j in range(minor - 1)
        ]

    greet(
        [partner] + [{"yr": c * 2 + core} for c in chip_at[1:]] + near_peers,
        [
            (can_up, {"sta": (row + 1) * minor + place}),
            (can_down, {"sta": (row - 1) * minor + place}),
        ],
        (2 * (major - 1) - row) // major + (row + major - 1) // major,
    )

    pairs = []
    for k in [*range(1, chips), 0]:
        copy = remote(
            sums_ref.at[chip_at[k] * 2 + 1 - core], pair.at[k],
            pair_send.at[k], pair_recv.at[k], partner,
        )
        copy.start()
        pairs.append(copy)
    crossing = []
    for k in range(1, chips):
        pairs[k - 1].wait_recv()
        partial[k - 1] = sums_ref[chip_at[k] * 2 + core] + pair[k]
        copy = remote(
            partial.at[k - 1], across.at[k - 1], across_send.at[k - 1], across_recv.at[k - 1],
            {"yr": chip_at[k] * 2 + core},
        )
        copy.start()
        crossing.append(copy)
    pairs[-1].wait_recv()
    total = sums_ref[yr] + pair[0]
    for k, copy in enumerate(crossing):
        copy.wait_recv()
        total = total + across[k]
    out_ref[sta, :stations] = total
    out_ref[sta, stations:] = cells_ref[...]

    for able, copy_of in ((can_up, up), (can_down, down)):
        @pl.when(able)
        def _():
            copy_of(1).start()
    for copy in near(0, 0):
        copy.start()
    for d in range(1, major):
        for side, have, able, copy_of in (
            (0, row >= d, can_up, up), (1, row + d < major, can_down, down)
        ):
            @pl.when(have)
            def _():
                copy_of(d).wait_recv()
                if d + 1 < major:
                    @pl.when(able)
                    def _():
                        copy_of(d + 1).start()
                for copy in near(side, d):
                    copy.start()
    for copy in near(0, 0):
        copy.wait()
    for d in range(1, major):
        for side, have, able, copy_of in (
            (0, row >= d, can_up, up), (1, row + d < major, can_down, down)
        ):
            @pl.when(have)
            def _():
                for copy in near(side, d):
                    copy.wait()
            reach = (row >= d - 1) if side == 0 else (row + d - 1 < major)

            @pl.when(reach & able)
            def _():
                copy_of(d).wait_send()
    for copy in pairs + crossing:
        copy.wait_send()


def exchange_in(sums, cells, owners, ranges):
    stations = sums.shape[1]
    major = 4 if owners % 4 == 0 else owners
    chips, minor = ranges // 2, owners // major
    block = stations + cells.shape[0]
    dma = pltpu.SemaphoreType.DMA
    hops, near_count = max(major - 1, 1), max(minor - 1, 1)
    crossings = max(chips - 1, 1)
    return pl.pallas_call(
        functools.partial(gather_kernel, owners, ranges, major),
        in_specs=[pl.BlockSpec(memory_space=pltpu.VMEM)] * 2,
        out_specs=pl.BlockSpec(memory_space=pltpu.VMEM),
        out_shape=jax.ShapeDtypeStruct((owners, block, LANES), F32),
        scratch_shapes=[
            pltpu.VMEM((chips, stations, LANES), F32),
            pltpu.VMEM((crossings, stations, LANES), F32),
            pltpu.VMEM((crossings, stations, LANES), F32),
            dma((chips,)), dma((chips,)), dma((crossings,)), dma((crossings,)),
            dma((2, hops)), dma((2, hops)), dma((2, major, near_count)), dma((2, major, near_count)),
        ],
        compiler_params=pltpu.CompilerParams(
            collective_id=0, has_side_effects=True, vmem_limit_bytes=48 * 1024 * 1024
        ),
    )(sums, cells)


def per_device(temps, day_bits, block_offset, block_counts, station_cell):
    owners, ranges = lax.axis_size("sta"), lax.axis_size("yr")
    stations = station_cell.shape[0]
    block_total, day_count = temps.shape
    cell_dev = CELLS // owners
    cell_pad = round_up(cell_dev, 8 * ranges)
    packed = ranges * MOST_BLOCKS < 256
    rows = 1024 if block_total % 1024 == 0 else block_total
    offsets = block_offset.reshape(1, block_total)
    row_specs = [
        pl.BlockSpec((rows, day_count), lambda i: (i, 0)),
        pl.BlockSpec((day_bits.shape[0], rows), lambda i: (0, i)),
        pl.BlockSpec((1, rows), lambda i: (0, i)),
        pl.BlockSpec((1, stations), lambda i: (0, 0)),
    ]
    params = pltpu.CompilerParams(
        dimension_semantics=("arbitrary",), vmem_limit_bytes=48 * 1024 * 1024
    )
    sums = pl.pallas_call(
        functools.partial(sums_kernel, ranges, packed),
        grid=(block_total // rows,),
        in_specs=row_specs,
        out_specs=pl.BlockSpec((ranges, stations, LANES), lambda i: (0, 0, 0)),
        out_shape=jax.ShapeDtypeStruct((ranges, stations, LANES), F32),
        scratch_shapes=[
            pltpu.VMEM((3 * stations, 3 * LANES), F32),
            pltpu.VMEM((2, stations, LANES), jnp.int32),
        ],
        compiler_params=params,
    )(temps, day_bits, offsets, block_counts)

    cell_row_count = round_up(stations // LANES, 8)
    cell_rows = jnp.pad(
        station_cell.astype(F32).reshape(stations // LANES, LANES),
        ((0, cell_row_count - stations // LANES), (0, 0)),
    )
    got = exchange_in(sums, cell_rows, owners, ranges)

    part_rows = (cell_pad + stations) // ranges
    chunks = cell_chunks(ranges, cell_pad, stations)
    most = max(high - low for low, high in chunks)
    columns = (3 if packed else 4) * LANES
    dma = pltpu.SemaphoreType.DMA
    hops = (len(chunks), max(ranges // 2 - 1, 1))
    steps = (len(chunks), ranges // 2)
    parts = pl.pallas_call(
        functools.partial(cells_kernel, ranges, packed, cell_dev, cell_pad),
        in_specs=[pl.BlockSpec(memory_space=pltpu.VMEM)] * 2,
        out_specs=pl.BlockSpec(memory_space=pltpu.VMEM),
        out_shape=jax.ShapeDtypeStruct((ranges, 3, part_rows, LANES), F32),
        scratch_shapes=[
            pltpu.VMEM((owners * stations, columns), BF16),
            pltpu.VMEM((ranges * most, columns), F32),
            dma(hops), dma(hops), dma(steps), dma(steps),
        ],
        compiler_params=pltpu.CompilerParams(
            collective_id=1, has_side_effects=True, vmem_limit_bytes=48 * 1024 * 1024
        ),
    )(got, station_cell.astype(F32).reshape(stations, 1))

    return pl.pallas_call(
        functools.partial(anomaly_kernel, ranges, cell_dev, cell_pad),
        grid=(block_total // rows,),
        in_specs=row_specs
        + [pl.BlockSpec((ranges, 3, part_rows, LANES), lambda i: (0, 0, 0, 0))],
        out_specs=[
            pl.BlockSpec((rows, day_count), lambda i: (i, 0)),
            pl.BlockSpec((cell_dev, 3 * LANES), lambda i: (0, 0)),
        ],
        out_shape=[
            jax.ShapeDtypeStruct((block_total, day_count), F32),
            jax.ShapeDtypeStruct((cell_dev, 3 * LANES), F32),
        ],
        scratch_shapes=[
            pltpu.VMEM((8, stations), jnp.int32),
            pltpu.VMEM((stations, 6 * LANES), BF16),
        ],
        compiler_params=params,
    )(temps, day_bits, offsets, block_counts, parts)


def solution(mesh):
    in_specs = (
        P(("sta", "yr"), None),
        P(None, ("sta", "yr")),
        P(("sta", "yr")),
        P("yr", "sta"),
        P("sta"),
    )
    out_specs = (P(("sta", "yr"), None), P("sta", None))

    def run(*args):
        return tuple(per_device(*args))

    return jax.shard_map(
        run, mesh=mesh, in_specs=in_specs, out_specs=out_specs, check_vma=False
    )
```
